32 devices in a mesh: grp: 2 (over y), user: 8 (over z, core), head: 2 (over x).
Axes of the slice: x: 2, y: 2, z: 4, core: 2. Of those that a mesh axis runs over, the one named last changes fastest.
Arguments:
- cand_ids: int32 [16, 512], P(('grp', 'user')), parts along dimension 0, may hold values from 0 to 4095, as said below
- prefix_len: int32 [16], P(('grp', 'user')), parts along dimension 0, may hold values from 1 to 512
- key_cache: bfloat16 [16, 512, 1024], P(('grp', 'user'), None, 'head'), parts along dimension 0, may hold values from -6 to 6
- value_cache: bfloat16 [16, 512, 1024], P(('grp', 'user'), None, 'head'), parts along dimension 0, may hold values from -6 to 6
- item_table: bfloat16 [4096, 1024], P('user'), may hold values from -6 to 6
- w_qkvu: bfloat16 [1024, 8, 4, 128], P(None, 'head'), may hold values from -0.1875 to 0.1875
- w_out: bfloat16 [8, 128, 1024], P('head'), may hold values from -0.1875 to 0.1875
Outputs:
- scores: float32 [16, 512], P(('grp', 'user')), parts along dimension 0
The draws below stay inside these ranges and needn't reach their ends.
There are 2 independent parts, one for each index of `grp`. The reference program is written for one: setup_inputs(seed, part) draws one part's arguments, and reference() takes and returns one part's arrays. A program takes and returns all parts, laid end to end along the dimension named above; an argument that names none is the same for every part. Nothing has to cross between parts.
Inputs may be any that keep to these rules, and one draw needn't show every extreme that they name: `cand_ids`: item id s * 512 + r lies in table shard s. Among the 512 candidates of each aligned block of 1 users, at most 128 lie in one table shard, and in every block some shard holds exactly 128 of them.
All inputs are finite; a program needn't handle non-finite values.
Results may differ from the reference program's by a relative error of at most 0.0095.
Values may be sent and summed in bfloat16 or wider, within the bound.
A program may use at most 64 MiB of HBM per device.

```python
import jax
import jax.numpy as jnp
from jax import lax

D = 1024
HEADS = 8
HD = 128
USR_DEV = 1
CAND = 512
PREF = 512
ROWS_SHARD = 512
USERS = 8
ITEMS = 4096
N_USER = 8
N_HEAD = 2


def draw_block(key):
    key_full, key_perm, key_shuffle, key_offset = jax.random.split(key, 4)
    row_count = USR_DEV * CAND
    capacity = 2 * row_count // N_USER
    slot_count = N_USER * capacity
    shard_ids = jnp.arange(slot_count, dtype=jnp.int32) // capacity
    full_shard = jax.random.randint(key_full, (), 0, N_USER, dtype=jnp.int32)
    permuted = jax.random.permutation(key_perm, slot_count).astype(jnp.int32)
    priority = permuted + jnp.where(shard_ids == full_shard, slot_count, 0).astype(jnp.int32)
    ordering = jnp.argsort(-priority, stable=True)
    chosen = shard_ids[ordering[:row_count]]
    chosen = jax.random.permutation(key_shuffle, chosen)
    offsets = jax.random.randint(key_offset, (row_count,), 0, ROWS_SHARD, dtype=jnp.int32)
    return (chosen * ROWS_SHARD + offsets).astype(jnp.int32)


def draw_cand_ids(key, part):
    block_keys = jax.random.split(jax.random.fold_in(key, 71), N_USER)
    blocks = jax.vmap(draw_block)(block_keys)
    return blocks.reshape(USR_DEV * N_USER, CAND).astype(jnp.int32)


def set_ends(entries, own_key, low, largest):
    spot = [jax.random.randint(jax.random.fold_in(own_key, axis), (), 0, length) for axis, length in enumerate(entries.shape)]
    widest = entries.shape.index(max(entries.shape))
    neighbour = spot[:widest] + [(spot[widest] + 1) % entries.shape[widest]] + spot[widest + 1:]
    return entries.at[tuple(spot)].set(low).at[tuple(neighbour)].set(largest)


def level_of(stream_key, extent, shards, low, largest):
    def one(position, parts):
        heights = jax.random.uniform(jax.random.fold_in(jax.random.fold_in(stream_key, 6), position), (parts,), jnp.float32, low / len(shards), largest / len(shards))
        return jnp.repeat(jnp.exp(heights), extent[position] // parts).reshape((-1,) + (1,) * (len(extent) - position - 1))

    factor_of = one(*shards[0])
    for cut in shards[1:]:
        factor_of = factor_of * one(*cut)
    return factor_of


def bell_draw(rng, dims, deviation, limit, cuts=(), held_as=jnp.bfloat16):
    entries = jax.random.normal(rng, dims, jnp.float32) * deviation
    if len(cuts) > 0:
        entries = level_of(rng, dims, cuts, -0.22, 0.18) * entries
    return jnp.clip(entries, min=-limit, max=limit).astype(held_as)


def setup_inputs(seed: int = 0, part: int = 0) -> dict:
    keys = jax.random.split(jax.random.key(seed), 8)
    part_keys = jax.random.split(jax.random.fold_in(keys[7], part), 8)
    cand_ids = draw_cand_ids(jax.random.fold_in(jax.random.fold_in(keys[7], part), 71), part)
    prefix_len = set_ends(jax.random.randint(part_keys[1], (USERS,), 1, PREF + 1), jax.random.fold_in(part_keys[1], 1), 1, PREF).astype(jnp.int32)
    key_cache = bell_draw(part_keys[2], (USERS, PREF, D), 1.0, 6.0, ((0, 8), (2, 2)))
    value_cache = bell_draw(part_keys[3], (USERS, PREF, D), 1.0, 6.0, ((0, 8), (2, 2)))
    item_table = bell_draw(keys[4], (ITEMS, D), 1.0, 6.0, ((0, 8),))
    w_qkvu = bell_draw(keys[5], (D, HEADS, 4, HD), D ** -0.5, 0.1875, ((1, 2),))
    w_out = bell_draw(keys[6], (HEADS, HD, D), D ** -0.5, 0.1875, ((0, 2),))
    return {"cand_ids": cand_ids, "prefix_len": prefix_len, "key_cache": key_cache, "value_cache": value_cache, "item_table": item_table, "w_qkvu": w_qkvu, "w_out": w_out}


def reference(cand_ids, prefix_len, key_cache, value_cache, item_table, w_qkvu, w_out):
    score_scale = HD ** (-0.5)
    flat_weight = w_qkvu.reshape(D, HEADS * 4 * HD)
    group_width = HEADS // N_HEAD * HD
    w_groups = w_out.reshape(N_HEAD, group_width, D).astype(jnp.float32)

    def one_user(packed):
        item_ids, length, cached_keys, cached_values = packed
        embedded = item_table[item_ids.astype(jnp.int32)]
        projected = jnp.dot(embedded, flat_weight, preferred_element_type=jnp.float32)
        activated = jax.nn.silu(projected).astype(jnp.bfloat16).reshape(CAND, HEADS, 4, HD)
        queries = activated[:, :, 0].astype(jnp.float32)
        own_keys = activated[:, :, 1].astype(jnp.float32)
        own_values = activated[:, :, 2].astype(jnp.float32)
        gates = activated[:, :, 3].astype(jnp.float32)
        keys_all = cached_keys.reshape(PREF, HEADS, HD).astype(jnp.float32)
        values_all = cached_values.reshape(PREF, HEADS, HD).astype(jnp.float32)
        raw = jnp.einsum('chd,phd->hcp', queries, keys_all)
        denominator = (length + 1).astype(jnp.float32)
        in_prefix = jnp.arange(PREF, dtype=jnp.int32) < length
        weights = jnp.where(in_prefix[None, None, :], jax.nn.silu(raw * score_scale), 0.0) / denominator
        weights = weights.astype(jnp.bfloat16).astype(jnp.float32)
        attended = jnp.einsum('hcp,phd->chd', weights, values_all)
        own_weight = jax.nn.silu(lax.optimization_barrier(jnp.sum(queries * own_keys, axis=-1)) * score_scale) / denominator
        attended = attended + own_weight[:, :, None] * own_values
        mean_square = lax.optimization_barrier(jnp.mean(attended * attended, axis=-1, keepdims=True))
        gated = (attended * lax.rsqrt(mean_square + 1e-06) * gates).astype(jnp.bfloat16)
        group_rows = gated.reshape(CAND, N_HEAD, group_width).astype(jnp.float32)
        partial_value = jnp.einsum('cgk,gkd->gcd', group_rows, w_groups).astype(jnp.bfloat16)
        summed = lax.optimization_barrier(jnp.sum(partial_value.astype(jnp.float32), axis=0))
        inner = lax.optimization_barrier(jnp.sum(summed * embedded.astype(jnp.float32), axis=-1)) * D ** (-0.5)
        return inner * lax.rsqrt(lax.optimization_barrier(jnp.mean(summed * summed, axis=-1)) + 1e-06)
    return lax.map(one_user, (cand_ids, prefix_len, key_cache, value_cache))
```

```python
import functools

import jax
import jax.numpy as jnp
from jax import lax
from jax.experimental import pallas as pl
from jax.experimental.pallas import tpu as pltpu
from jax.sharding import PartitionSpec as P

MESH = pl.DeviceIdType.MESH
PIECES = 2


def silu(v):
    return v * (0.5 * jnp.tanh(0.5 * v) + 0.5)


def kernel(
    chips, prefix_ref, ids_ref, key_hbm, value_hbm, table_hbm, w_hbm, wout_hbm, out_ref,
    tab, ids_peer, ids_wide, picked, one_hot, emb, emb_peer, w, keys, values, wout, acc, gated,
    gated_peer, halves, local_sem, z_send, z_recv, ids_sem, exch_send, exch_recv, wout_sem, tail_sem,
):
    grp, user, head = lax.axis_index("grp"), lax.axis_index("user"), lax.axis_index("head")
    z, core = user // 2, user % 2
    sibling = user + 1 - 2 * core
    quarter = 2 * grp + head
    shards, rows, width = tab.shape
    cand = ids_ref.shape[1]
    half = cand // 2
    piece = rows // PIECES
    heads, head_size = wout_hbm.shape[0], wout_hbm.shape[1]
    here = heads * head_size
    prefix_most = keys.shape[0]
    model = w.shape[0]
    x_peer = (grp, user, 1 - head)
    y_peer = (1 - grp, user, head)
    corner = (1 - grp, user, 1 - head)

    own = pltpu.make_async_copy(
        table_hbm.at[:, pl.ds(pl.multiple_of(quarter * width, width), width)],
        tab.at[user], local_sem.at[0],
    )
    loads = [
        pltpu.make_async_copy(wout_hbm, wout.at[head], local_sem.at[1]),
        pltpu.make_async_copy(w_hbm, w, local_sem.at[2]),
        pltpu.make_async_copy(key_hbm.at[0], keys, local_sem.at[3]),
        pltpu.make_async_copy(value_hbm.at[0], values, local_sem.at[4]),
    ]
    own.start()
    for load in loads:
        load.start()

    barrier = pltpu.get_barrier_semaphore()

    def greet(device):
        pl.semaphore_signal(barrier, inc=1, device_id=device, device_id_type=MESH)

    for device in ((grp, sibling, head), x_peer, y_peer, corner):
        greet(device)

    @pl.when(z > 0)
    def _():
        greet((grp, user - 2, head))

    @pl.when(z < chips - 1)
    def _():
        greet((grp, user + 2, head))

    pl.semaphore_wait(barrier, 4 + jnp.minimum(z, 1) + jnp.minimum(chips - 1 - z, 1))

    def remote(src, dst, send, recv, device):
        return pltpu.make_async_remote_copy(
            src_ref=src, dst_ref=dst, send_sem=send, recv_sem=recv, device_id=device,
            device_id_type=MESH,
        )

    def block(chip, parity, part):
        return tab.at[2 * chip + parity, pl.ds(part * piece, piece)]

    def along(chip, part, step):
        place = block(chip, core, part)
        return remote(
            place, place, z_send.at[0 if step > 0 else 1, chip, part], z_recv.at[0, chip, part],
            (grp, user + 2 * step, head),
        )

    def across(chip, part, parity):
        place = block(chip, parity, part)
        return remote(
            place, place, z_send.at[2, chip, part], z_recv.at[1, chip, part],
            (grp, sibling, head),
        )

    def when(condition, action):
        pl.when(condition)(action)

    ids_copy = remote(ids_ref, ids_peer, ids_sem.at[0], ids_sem.at[1], y_peer)
    ids_copy.start()
    own.wait()
    for part in range(PIECES):
        when(z < chips - 1, lambda: along(z, part, 1).start())
        when(z > 0, lambda: along(z, part, -1).start())
        across(z, part, core).start()
    loads[0].wait()
    wout_copies = []
    depth = head_size * heads // 2

    def wout_part(group, part):
        return wout.at[group, pl.ds(pl.multiple_of(part * (heads // 2), heads // 2), heads // 2)]

    to_peer = remote(wout_part(head, core), wout_part(head, core), wout_sem.at[0], wout_sem.at[1], x_peer)
    to_peer.start()
    ids_copy.wait()

    lane = lax.broadcasted_iota(jnp.int32, (cand, 128), 1)
    diagonal = lax.broadcasted_iota(jnp.int32, (cand, cand), 0) == lax.broadcasted_iota(
        jnp.int32, (cand, cand), 1
    )
    for which, source in enumerate((ids_ref, ids_peer)):
        column = jnp.sum(
            jnp.where(diagonal, source[...].astype(jnp.float32), 0.0), axis=1, keepdims=True
        ).astype(jnp.int32)
        ids_wide[which] = jnp.broadcast_to(column, (cand, 128))
    picked[...] = jnp.zeros_like(picked)

    def pick(chip):
        def step(i, carry):
            which, parity = i // 2, i % 2
            shard = 2 * chip + parity
            wide = ids_wide[which] - shard * rows
            for j in range(rows // 128):
                one_hot[:, j * 128 : (j + 1) * 128] = jnp.where(
                    wide == lane + j * 128, 1.0, 0.0
                ).astype(jnp.bfloat16)
            picked[which] += jnp.dot(
                one_hot[...], tab[shard], preferred_element_type=jnp.float32
            )
            return carry

        lax.fori_loop(0, 4, step, 0)

    def take(chip):
        for part in range(PIECES):
            across(chip, part, 1 - core).wait_recv()
        pick(chip)

    take(z)
    for distance in range(1, chips):
        for part in range(PIECES):

            @pl.when(z - distance >= 0)
            def _():
                along(z - distance, part, 1).wait_recv()
                when(z < chips - 1, lambda: along(z - distance, part, 1).start())
                across(z - distance, part, core).start()

            @pl.when(z + distance < chips)
            def _():
                along(z + distance, part, -1).wait_recv()
                when(z > 0, lambda: along(z + distance, part, -1).start())
                across(z + distance, part, core).start()

        when(z - distance >= 0, lambda: take(z - distance))
        when(z + distance < chips, lambda: take(z + distance))

    emb[quarter] = picked[0].astype(jnp.bfloat16)
    emb_peer[...] = picked[1].astype(jnp.bfloat16)
    exchange = [
        remote(emb.at[quarter], emb.at[quarter], exch_send.at[0], exch_recv.at[quarter], x_peer),
        remote(emb_peer, emb.at[quarter], exch_send.at[1], exch_recv.at[quarter], y_peer),
        remote(emb_peer, emb.at[quarter], exch_send.at[2], exch_recv.at[quarter], corner),
    ]
    for copy in exchange:
        copy.start()
    to_peer.wait()
    forward = remote(
        wout_part(1 - head, core), wout_part(1 - head, core), wout_sem.at[2], wout_sem.at[3],
        (grp, sibling, head),
    )
    forward.start()
    for load in loads[1:]:
        load.wait()

    def weight(which, h):
        return w[
            pl.ds(pl.multiple_of(which * width, width), width),
            pl.ds(pl.multiple_of(h * 4 * head_size, 4 * head_size), 4 * head_size),
        ]

    def embedded(which, r):
        return emb[which, pl.ds(pl.multiple_of(r * half, half), half)]

    def project(which, r, h):
        return jnp.dot(embedded(which, r), weight(which, h), preferred_element_type=jnp.float32)

    def arrived(which):
        remote(
            emb.at[which], emb.at[which], exch_send.at[0], exch_recv.at[which], x_peer
        ).wait_recv()

    x_quarter, y_quarter = 2 * grp + 1 - head, 2 * (1 - grp) + head
    corner_quarter = 2 * (1 - grp) + 1 - head

    def first(i, carry):
        acc[i // heads, i % heads] = project(quarter, i // heads, i % heads)
        return carry

    lax.fori_loop(0, 2 * heads, first, 0)
    for which in (x_quarter, y_quarter):
        arrived(which)

        def add(i, carry):
            acc[i // heads, i % heads] += project(which, i // heads, i % heads)
            return carry

        lax.fori_loop(0, 2 * heads, add, 0)
    arrived(corner_quarter)

    length = prefix_ref[0]
    inverse = 1.0 / (length + 1).astype(jnp.float32)
    in_prefix = lax.broadcasted_iota(jnp.int32, (1, prefix_most), 1) < length
    factor = jnp.where(in_prefix, inverse, 0.0)
    scale = head_size ** (-0.5)

    def attend(r):
        def step(h, carry):
            activated = silu(acc[r, h] + project(corner_quarter, r, h)).astype(jnp.bfloat16)
            query, own_key, own_value, gate = (
                activated[:, j * head_size : (j + 1) * head_size] for j in range(4)
            )
            columns = pl.ds(pl.multiple_of(h * head_size, head_size), head_size)
            raw = lax.dot_general(
                query, keys[:, columns], (((1,), (1,)), ((), ())),
                preferred_element_type=jnp.float32,
            )
            weights = (silu(raw * scale) * factor).astype(jnp.bfloat16)
            attended = jnp.dot(weights, values[:, columns], preferred_element_type=jnp.float32)
            own_dot = jnp.sum(
                query.astype(jnp.float32) * own_key.astype(jnp.float32), axis=1, keepdims=True
            )
            attended += silu(own_dot * scale) * inverse * own_value.astype(jnp.float32)
            mean_square = jnp.mean(attended * attended, axis=1, keepdims=True)
            gated[r, :, columns] = (
                attended * lax.rsqrt(mean_square + 1e-06) * gate.astype(jnp.float32)
            ).astype(jnp.bfloat16)
            return carry

        lax.fori_loop(0, heads, step, 0)

    attend(1 - head)
    hand_over = remote(gated.at[1 - head], gated_peer, tail_sem.at[0], tail_sem.at[1], x_peer)
    hand_over.start()
    attend(head)
    forward.wait()

    def product(rows_here, group):
        return (
            jnp.dot(
                rows_here, wout[group].reshape(here, model), preferred_element_type=jnp.float32
            )
            .astype(jnp.bfloat16)
            .astype(jnp.float32)
        )

    summed = product(gated[head], head)
    hand_over.wait()
    summed += product(gated_peer[...], 1 - head)
    square = jnp.sum(summed * summed, axis=1, keepdims=True)
    inner = sum(
        jnp.sum(
            summed[:, i * width : (i + 1) * width] * embedded(i, head).astype(jnp.float32),
            axis=1, keepdims=True,
        )
        for i in range(model // width)
    )
    score = inner * model ** (-0.5) * lax.rsqrt(square / model + 1e-06)
    halves[head] = jnp.sum(jnp.where(diagonal[:half, :half], score, 0.0), axis=0, keepdims=True)
    last = remote(halves.at[head], halves.at[head], tail_sem.at[2], tail_sem.at[3], x_peer)
    last.start()
    for part in range(PIECES):
        for chip in range(chips):

            @pl.when(z < chips - 1)
            def _():
                when(chip <= z, lambda: along(chip, part, 1).wait_send())

            @pl.when(z > 0)
            def _():
                when(chip >= z, lambda: along(chip, part, -1).wait_send())

            across(chip, part, core).wait_send()
    for copy in exchange:
        copy.wait_send()
    last.wait()
    for i in range(2):
        out_ref[:, i * half : (i + 1) * half] = halves[i]


def fused_body(mesh, cand_ids, prefix_len, key_cache, value_cache, item_table, w_qkvu, w_out):
    cand = cand_ids.shape[1]
    rows, model = item_table.shape
    heads, head_size = w_qkvu.shape[1], w_qkvu.shape[3]
    prefix_most, here = key_cache.shape[1:]
    shards = mesh.shape["user"]
    chips = shards // 2
    width = model // 4
    half = cand // 2
    hbm = pl.BlockSpec(memory_space=pl.ANY)
    bf16, f32 = jnp.bfloat16, jnp.float32
    return pl.pallas_call(
        functools.partial(kernel, chips),
        out_shape=jax.ShapeDtypeStruct((1, cand), f32),
        in_specs=[
            pl.BlockSpec(memory_space=pltpu.SMEM), pl.BlockSpec(memory_space=pltpu.VMEM),
            hbm, hbm, hbm, hbm, hbm,
        ],
        out_specs=pl.BlockSpec(memory_space=pltpu.VMEM),
        scratch_shapes=[
            pltpu.VMEM((shards, rows, width), bf16),
            pltpu.VMEM((1, cand), jnp.int32),
            pltpu.VMEM((2, cand, 128), jnp.int32),
            pltpu.VMEM((2, cand, width), f32),
            pltpu.VMEM((cand, rows), bf16),
            pltpu.VMEM((4, cand, width), bf16),
            pltpu.VMEM((cand, width), bf16),
            pltpu.VMEM((model, heads * 4 * head_size), bf16),
            pltpu.VMEM((prefix_most, here), bf16),
            pltpu.VMEM((prefix_most, here), bf16),
            pltpu.VMEM((2, heads, head_size, model), bf16),
            pltpu.VMEM((2, heads, half, 4 * head_size), f32),
            pltpu.VMEM((2, half, here), bf16),
            pltpu.VMEM((half, here), bf16),
            pltpu.VMEM((2, 1, half), f32),
            pltpu.SemaphoreType.DMA((5,)),
            pltpu.SemaphoreType.DMA((3, chips, PIECES)),
            pltpu.SemaphoreType.DMA((2, chips, PIECES)),
            pltpu.SemaphoreType.DMA((2,)),
            pltpu.SemaphoreType.DMA((3,)),
            pltpu.SemaphoreType.DMA((4,)),
            pltpu.SemaphoreType.DMA((4,)),
            pltpu.SemaphoreType.DMA((4,)),
        ],
        compiler_params=pltpu.CompilerParams(
            collective_id=0, has_side_effects=True, vmem_limit_bytes=60 * 1024 * 1024
        ),
    )(
        prefix_len, cand_ids, key_cache, value_cache, item_table,
        w_qkvu.reshape(model, heads * 4 * head_size), w_out,
    )


def fits_fused(mesh):
    shape = mesh.shape
    return shape["grp"] == 2 and shape["head"] == 2 and shape["user"] % 2 == 0 and shape["user"] <= 8


def fused(mesh):
    in_specs = (
        P(("grp", "user"), None),
        P(("grp", "user")),
        P(("grp", "user"), None, "head"),
        P(("grp", "user"), None, "head"),
        P("user", None),
        P(None, "head", None, None),
        P("head", None, None),
    )
    return jax.shard_map(
        functools.partial(fused_body, mesh), mesh=mesh, in_specs=in_specs,
        out_specs=P(("grp", "user"), None), check_vma=False,
    )


def body(cand_ids, prefix_len, key_cache, value_cache, item_table, w_qkvu, w_out):
    user_count, cand_count = cand_ids.shape
    model_width = item_table.shape[1]
    heads_here = w_qkvu.shape[1]
    head_size = w_qkvu.shape[3]
    prefix_most = key_cache.shape[1]
    score_scale = head_size ** (-0.5)
    shard_count = lax.axis_size("user")
    rows_shard = item_table.shape[0]
    item_ids = cand_ids.reshape(-1)
    row_count = item_ids.shape[0]
    capacity = 2 * row_count // shard_count
    shard_of = item_ids // rows_shard
    local_row = item_ids - shard_of * rows_shard
    one_hot = (shard_of[:, None] == jnp.arange(shard_count, dtype=jnp.int32)[None, :]).astype(
        jnp.int32
    )
    position = jnp.sum((jnp.cumsum(one_hot, axis=0) - 1) * one_hot, axis=1)
    slot_index = shard_of * capacity + position
    requests = jnp.full((shard_count * capacity,), -1, jnp.int32).at[slot_index].set(local_row)
    received = lax.all_to_all(
        requests.reshape(shard_count, capacity), "user", split_axis=0, concat_axis=0, tiled=True
    )
    safe_rows = jnp.maximum(received.reshape(-1), 0)
    looked_up = item_table[safe_rows].reshape(shard_count, capacity, model_width)
    returned = lax.all_to_all(looked_up, "user", split_axis=0, concat_axis=0, tiled=True)
    embedded = returned.reshape(-1, model_width)[slot_index]
    projected = jnp.dot(
        embedded, w_qkvu.reshape(model_width, -1), preferred_element_type=jnp.float32
    )
    activated = jax.nn.silu(projected).astype(jnp.bfloat16)
    activated = activated.reshape(user_count, cand_count, heads_here, 4, head_size)
    queries = activated[:, :, :, 0]
    own_keys = activated[:, :, :, 1]
    own_values = activated[:, :, :, 2]
    gates = activated[:, :, :, 3]
    cached_keys = key_cache.reshape(user_count, prefix_most, heads_here, head_size)
    cached_values = value_cache.reshape(user_count, prefix_most, heads_here, head_size)
    raw = jnp.einsum("uchd,uphd->uhcp", queries, cached_keys, preferred_element_type=jnp.float32)
    denominator = (prefix_len + 1).astype(jnp.float32)
    in_prefix = jnp.arange(prefix_most, dtype=jnp.int32)[None, :] < prefix_len[:, None]
    weights = jnp.where(in_prefix[:, None, None, :], jax.nn.silu(raw * score_scale), 0.0)
    weights = (weights / denominator[:, None, None, None]).astype(jnp.bfloat16)
    attended = jnp.einsum(
        "uhcp,uphd->uchd", weights, cached_values, preferred_element_type=jnp.float32
    )
    own_dot = jnp.sum(queries.astype(jnp.float32) * own_keys.astype(jnp.float32), axis=-1)
    own_weight = jax.nn.silu(own_dot * score_scale) / denominator[:, None, None]
    attended = attended + own_weight[..., None] * own_values.astype(jnp.float32)
    mean_square = jnp.mean(attended * attended, axis=-1, keepdims=True)
    gated = (attended * lax.rsqrt(mean_square + 1e-06) * gates.astype(jnp.float32)).astype(
        jnp.bfloat16
    )
    partial_value = jnp.dot(
        gated.reshape(row_count, heads_here * head_size),
        w_out.reshape(heads_here * head_size, model_width),
        preferred_element_type=jnp.float32,
    )
    col_width = model_width // lax.axis_size("head")
    head_index = lax.axis_index("head")
    summed_cols = lax.psum_scatter(
        partial_value.astype(jnp.bfloat16), "head", scatter_dimension=1, tiled=True
    ).astype(jnp.float32)
    embed_cols = lax.dynamic_slice_in_dim(embedded, head_index * col_width, col_width, 1).astype(
        jnp.float32
    )
    square_part = jnp.sum(summed_cols * summed_cols, axis=1)
    inner_part = jnp.sum(summed_cols * embed_cols, axis=1)
    square_total, inner_total = lax.psum((square_part, inner_part), "head")
    scores_out = inner_total * model_width ** (-0.5) * lax.rsqrt(square_total / model_width + 1e-06)
    return scores_out.reshape(user_count, cand_count)


def solution(mesh):
    if fits_fused(mesh):
        return fused(mesh)
    in_specs = (
        P(("grp", "user"), None),
        P(("grp", "user")),
        P(("grp", "user"), None, "head"),
        P(("grp", "user"), None, "head"),
        P("user", None),
        P(None, "head", None, None),
        P("head", None, None),
    )
    out_specs = P(("grp", "user"), None)
    return jax.shard_map(body, mesh=mesh, in_specs=in_specs, out_specs=out_specs, check_vma=False)
```

```python
import functools

import jax
import jax.numpy as jnp
from jax import lax
from jax.experimental import pallas as pl
from jax.experimental.pallas import tpu as pltpu
from jax.sharding import PartitionSpec as P

MESH = pl.DeviceIdType.MESH
PIECES = 2
STRIP = 128


def silu(v):
    return v * (0.5 * jnp.tanh(0.5 * v) + 0.5)


def kernel(
    chips, prefix_ref, ids_ref, key_hbm, value_hbm, table_hbm, w_hbm, wout_hbm, out_ref,
    tab, ids_peer, ids_wide, picked, one_hot, emb, emb_peer, w_raw, w_wide, w, keys, values, wout, acc, gated,
    gated_peer, halves, local_sem, z_send, z_recv, ids_sem, exch_send, exch_recv, wout_sem, tail_sem,
):
    grp, user, head = lax.axis_index("grp"), lax.axis_index("user"), lax.axis_index("head")
    z, core = user // 2, user % 2
    sibling = user + 1 - 2 * core
    quarter = 2 * grp + head
    shards, rows, width = tab.shape
    cand = ids_ref.shape[1]
    half = cand // 2
    piece = rows // PIECES
    heads, head_size = wout_hbm.shape[0], wout_hbm.shape[1]
    here = heads * head_size
    prefix_most = keys.shape[0]
    model = w.shape[0]
    x_peer = (grp, user, 1 - head)
    y_peer = (1 - grp, user, head)
    corner = (1 - grp, user, 1 - head)

    own = pltpu.make_async_copy(
        table_hbm.at[:, pl.ds(pl.multiple_of(quarter * width, width), width)],
        tab.at[user], local_sem.at[0],
    )
    loads = [
        pltpu.make_async_copy(wout_hbm, wout.at[head], local_sem.at[1]),
        pltpu.make_async_copy(w_hbm, w_raw, local_sem.at[2]),
        pltpu.make_async_copy(key_hbm.at[0], keys, local_sem.at[3]),
        pltpu.make_async_copy(value_hbm.at[0], values, local_sem.at[4]),
    ]
    own.start()
    for load in loads:
        load.start()

    barrier = pltpu.get_barrier_semaphore()

    def greet(device):
        pl.semaphore_signal(barrier, inc=1, device_id=device, device_id_type=MESH)

    for device in ((grp, sibling, head), x_peer, y_peer, corner):
        greet(device)

    @pl.when(z > 0)
    def _():
        greet((grp, user - 2, head))

    @pl.when(z < chips - 1)
    def _():
        greet((grp, user + 2, head))

    pl.semaphore_wait(barrier, 4 + jnp.minimum(z, 1) + jnp.minimum(chips - 1 - z, 1))

    def remote(src, dst, send, recv, device):
        return pltpu.make_async_remote_copy(
            src_ref=src, dst_ref=dst, send_sem=send, recv_sem=recv, device_id=device,
            device_id_type=MESH,
        )

    def block(chip, parity, part):
        return tab.at[2 * chip + parity, pl.ds(part * piece, piece)]

    def along(chip, part, step):
        place = block(chip, core, part)
        return remote(
            place, place, z_send.at[0 if step > 0 else 1, chip, part], z_recv.at[0, chip, part],
            (grp, user + 2 * step, head),
        )

    def across(chip, part, parity):
        place = block(chip, parity, part)
        return remote(
            place, place, z_send.at[2, chip, part], z_recv.at[1, chip, part],
            (grp, sibling, head),
        )

    def when(condition, action):
        pl.when(condition)(action)

    ids_copy = remote(ids_ref, ids_peer, ids_sem.at[0], ids_sem.at[1], y_peer)
    ids_copy.start()
    own.wait()
    for part in range(PIECES):
        when(z < chips - 1, lambda: along(z, part, 1).start())
        when(z > 0, lambda: along(z, part, -1).start())
        across(z, part, core).start()
    loads[0].wait()
    wout_copies = []
    depth = head_size * heads // 2

    def wout_part(group, part):
        return wout.at[group, pl.ds(pl.multiple_of(part * (heads // 2), heads // 2), heads // 2)]

    to_peer = remote(wout_part(head, core), wout_part(head, core), wout_sem.at[0], wout_sem.at[1], x_peer)
    to_peer.start()
    ids_copy.wait()

    lane = lax.broadcasted_iota(jnp.int32, (cand, 128), 1)
    diagonal = lax.broadcasted_iota(jnp.int32, (cand, cand), 0) == lax.broadcasted_iota(
        jnp.int32, (cand, cand), 1
    )
    for which, source in enumerate((ids_ref, ids_peer)):
        column = jnp.sum(
            jnp.where(diagonal, source[...].astype(jnp.float32), 0.0), axis=1, keepdims=True
        ).astype(jnp.int32)
        ids_wide[which] = jnp.broadcast_to(column, (cand, 128))
    picked[...] = jnp.zeros_like(picked)

    def pick(chip):
        def step(i, carry):
            which, parity = i // 2, i % 2
            shard = 2 * chip + parity
            wide = ids_wide[which] - shard * rows
            for j in range(rows // 128):
                one_hot[:, j * 128 : (j + 1) * 128] = jnp.where(
                    wide == lane + j * 128, 1.0, 0.0
                ).astype(jnp.bfloat16)
            picked[which] += jnp.dot(
                one_hot[...], tab[shard], preferred_element_type=jnp.float32
            )
            return carry

        lax.fori_loop(0, 4, step, 0)

    def take(chip):
        for part in range(PIECES):
            across(chip, part, 1 - core).wait_recv()
        pick(chip)

    slots = heads * 4
    strips = model // STRIP

    def spread(i, carry):
        start = pl.multiple_of(i * STRIP * slots, STRIP * slots)
        w_wide[...] = w_raw[pl.ds(start, STRIP * slots)].astype(jnp.float32)
        for j in range(slots):
            w[pl.ds(pl.multiple_of(i * STRIP, STRIP), STRIP), j * head_size : (j + 1) * head_size] = (
                w_wide[pl.ds(j, STRIP, stride=slots)].astype(jnp.bfloat16)
            )
        return carry

    take(z)
    loads[1].wait()
    for distance in range(1, chips):
        lax.fori_loop(
            (distance - 1) * strips // (chips - 1), distance * strips // (chips - 1), spread, 0
        )
        for part in range(PIECES):

            @pl.when(z - distance >= 0)
            def _():
                along(z - distance, part, 1).wait_recv()
                when(z < chips - 1, lambda: along(z - distance, part, 1).start())
                across(z - distance, part, core).start()

            @pl.when(z + distance < chips)
            def _():
                along(z + distance, part, -1).wait_recv()
                when(z > 0, lambda: along(z + distance, part, -1).start())
                across(z + distance, part, core).start()

        when(z - distance >= 0, lambda: take(z - distance))
        when(z + distance < chips, lambda: take(z + distance))

    emb[quarter] = picked[0].astype(jnp.bfloat16)
    emb_peer[...] = picked[1].astype(jnp.bfloat16)
    exchange = [
        remote(emb.at[quarter], emb.at[quarter], exch_send.at[0], exch_recv.at[quarter], x_peer),
        remote(emb_peer, emb.at[quarter], exch_send.at[1], exch_recv.at[quarter], y_peer),
        remote(emb_peer, emb.at[quarter], exch_send.at[2], exch_recv.at[quarter], corner),
    ]
    for copy in exchange:
        copy.start()
    to_peer.wait()
    forward = remote(
        wout_part(1 - head, core), wout_part(1 - head, core), wout_sem.at[2], wout_sem.at[3],
        (grp, sibling, head),
    )
    forward.start()
    for load in loads[2:]:
        load.wait()

    def weight(which, h):
        return w[
            pl.ds(pl.multiple_of(which * width, width), width),
            pl.ds(pl.multiple_of(h * 4 * head_size, 4 * head_size), 4 * head_size),
        ]

    def embedded(which, r):
        return emb[which, pl.ds(pl.multiple_of(r * half, half), half)]

    def project(which, r, h):
        return jnp.dot(embedded(which, r), weight(which, h), preferred_element_type=jnp.float32)

    def arrived(which):
        remote(
            emb.at[which], emb.at[which], exch_send.at[0], exch_recv.at[which], x_peer
        ).wait_recv()

    x_quarter, y_quarter = 2 * grp + 1 - head, 2 * (1 - grp) + head
    corner_quarter = 2 * (1 - grp) + 1 - head

    def first(i, carry):
        acc[i // heads, i % heads] = project(quarter, i // heads, i % heads)
        return carry

    lax.fori_loop(0, 2 * heads, first, 0)
    for which in (x_quarter, y_quarter):
        arrived(which)

        def add(i, carry):
            acc[i // heads, i % heads] += project(which, i // heads, i % heads)
            return carry

        lax.fori_loop(0, 2 * heads, add, 0)
    arrived(corner_quarter)

    length = prefix_ref[0]
    inverse = 1.0 / (length + 1).astype(jnp.float32)
    in_prefix = lax.broadcasted_iota(jnp.int32, (1, prefix_most), 1) < length
    factor = jnp.where(in_prefix, inverse, 0.0)
    scale = head_size ** (-0.5)

    def attend(r):
        def step(h, carry):
            activated = silu(acc[r, h] + project(corner_quarter, r, h)).astype(jnp.bfloat16)
            query, own_key, own_value, gate = (
                activated[:, j * head_size : (j + 1) * head_size] for j in range(4)
            )
            columns = pl.ds(pl.multiple_of(h * head_size, head_size), head_size)
            raw = lax.dot_general(
                query, keys[:, columns], (((1,), (1,)), ((), ())),
                preferred_element_type=jnp.float32,
            )
            weights = (silu(raw * scale) * factor).astype(jnp.bfloat16)
            attended = jnp.dot(weights, values[:, columns], preferred_element_type=jnp.float32)
            own_dot = jnp.sum(
                query.astype(jnp.float32) * own_key.astype(jnp.float32), axis=1, keepdims=True
            )
            attended += silu(own_dot * scale) * inverse * own_value.astype(jnp.float32)
            mean_square = jnp.mean(attended * attended, axis=1, keepdims=True)
            gated[r, :, columns] = (
                attended * lax.rsqrt(mean_square + 1e-06) * gate.astype(jnp.float32)
            ).astype(jnp.bfloat16)
            return carry

        lax.fori_loop(0, heads, step, 0)

    attend(1 - head)
    hand_over = remote(gated.at[1 - head], gated_peer, tail_sem.at[0], tail_sem.at[1], x_peer)
    hand_over.start()
    attend(head)
    forward.wait()

    def product(rows_here, group):
        return (
            jnp.dot(
                rows_here, wout[group].reshape(here, model), preferred_element_type=jnp.float32
            )
            .astype(jnp.bfloat16)
            .astype(jnp.float32)
        )

    summed = product(gated[head], head)
    hand_over.wait()
    summed += product(gated_peer[...], 1 - head)
    square = jnp.sum(summed * summed, axis=1, keepdims=True)
    inner = sum(
        jnp.sum(
            summed[:, i * width : (i + 1) * width] * embedded(i, head).astype(jnp.float32),
            axis=1, keepdims=True,
        )
        for i in range(model // width)
    )
    score = inner * model ** (-0.5) * lax.rsqrt(square / model + 1e-06)
    halves[head] = jnp.sum(jnp.where(diagonal[:half, :half], score, 0.0), axis=0, keepdims=True)
    last = remote(halves.at[head], halves.at[head], tail_sem.at[2], tail_sem.at[3], x_peer)
    last.start()
    for part in range(PIECES):
        for chip in range(chips):

            @pl.when(z < chips - 1)
            def _():
                when(chip <= z, lambda: along(chip, part, 1).wait_send())

            @pl.when(z > 0)
            def _():
                when(chip >= z, lambda: along(chip, part, -1).wait_send())

            across(chip, part, core).wait_send()
    for copy in exchange:
        copy.wait_send()
    last.wait()
    for i in range(2):
        out_ref[:, i * half : (i + 1) * half] = halves[i]


def fused_body(mesh, cand_ids, prefix_len, key_cache, value_cache, item_table, w_qkvu, w_out):
    cand = cand_ids.shape[1]
    rows, model = item_table.shape
    heads, head_size = w_qkvu.shape[1], w_qkvu.shape[3]
    prefix_most, here = key_cache.shape[1:]
    shards = mesh.shape["user"]
    chips = shards // 2
    width = model // 4
    half = cand // 2
    hbm = pl.BlockSpec(memory_space=pl.ANY)
    bf16, f32 = jnp.bfloat16, jnp.float32
    return pl.pallas_call(
        functools.partial(kernel, chips),
        out_shape=jax.ShapeDtypeStruct((1, cand), f32),
        in_specs=[
            pl.BlockSpec(memory_space=pltpu.SMEM), pl.BlockSpec(memory_space=pltpu.VMEM),
            hbm, hbm, hbm, hbm, hbm,
        ],
        out_specs=pl.BlockSpec(memory_space=pltpu.VMEM),
        scratch_shapes=[
            pltpu.VMEM((shards, rows, width), bf16),
            pltpu.VMEM((1, cand), jnp.int32),
            pltpu.VMEM((2, cand, 128), jnp.int32),
            pltpu.VMEM((2, cand, width), f32),
            pltpu.VMEM((cand, rows), bf16),
            pltpu.VMEM((4, cand, width), bf16),
            pltpu.VMEM((cand, width), bf16),
            pltpu.VMEM((model * heads * 4, head_size), bf16),
            pltpu.VMEM((STRIP * heads * 4, head_size), f32),
            pltpu.VMEM((model, heads * 4 * head_size), bf16),
            pltpu.VMEM((prefix_most, here), bf16),
            pltpu.VMEM((prefix_most, here), bf16),
            pltpu.VMEM((2, heads, head_size, model), bf16),
            pltpu.VMEM((2, heads, half, 4 * head_size), f32),
            pltpu.VMEM((2, half, here), bf16),
            pltpu.VMEM((half, here), bf16),
            pltpu.VMEM((2, 1, half), f32),
            pltpu.SemaphoreType.DMA((5,)),
            pltpu.SemaphoreType.DMA((3, chips, PIECES)),
            pltpu.SemaphoreType.DMA((2, chips, PIECES)),
            pltpu.SemaphoreType.DMA((2,)),
            pltpu.SemaphoreType.DMA((3,)),
            pltpu.SemaphoreType.DMA((4,)),
            pltpu.SemaphoreType.DMA((4,)),
            pltpu.SemaphoreType.DMA((4,)),
        ],
        compiler_params=pltpu.CompilerParams(
            collective_id=0, has_side_effects=True, vmem_limit_bytes=60 * 1024 * 1024
        ),
    )(
        prefix_len, cand_ids, key_cache, value_cache, item_table,
        w_qkvu.reshape(model * heads * 4, head_size), w_out,
    )


def fits_fused(mesh):
    shape = mesh.shape
    return shape["grp"] == 2 and shape["head"] == 2 and shape["user"] % 2 == 0 and shape["user"] <= 8


def fused(mesh):
    in_specs = (
        P(("grp", "user"), None),
        P(("grp", "user")),
        P(("grp", "user"), None, "head"),
        P(("grp", "user"), None, "head"),
        P("user", None),
        P(None, "head", None, None),
        P("head", None, None),
    )
    return jax.shard_map(
        functools.partial(fused_body, mesh), mesh=mesh, in_specs=in_specs,
        out_specs=P(("grp", "user"), None), check_vma=False,
    )


def body(cand_ids, prefix_len, key_cache, value_cache, item_table, w_qkvu, w_out):
    user_count, cand_count = cand_ids.shape
    model_width = item_table.shape[1]
    heads_here = w_qkvu.shape[1]
    head_size = w_qkvu.shape[3]
    prefix_most = key_cache.shape[1]
    score_scale = head_size ** (-0.5)
    shard_count = lax.axis_size("user")
    rows_shard = item_table.shape[0]
    item_ids = cand_ids.reshape(-1)
    row_count = item_ids.shape[0]
    capacity = 2 * row_count // shard_count
    shard_of = item_ids // rows_shard
    local_row = item_ids - shard_of * rows_shard
    one_hot = (shard_of[:, None] == jnp.arange(shard_count, dtype=jnp.int32)[None, :]).astype(
        jnp.int32
    )
    position = jnp.sum((jnp.cumsum(one_hot, axis=0) - 1) * one_hot, axis=1)
    slot_index = shard_of * capacity + position
    requests = jnp.full((shard_count * capacity,), -1, jnp.int32).at[slot_index].set(local_row)
    received = lax.all_to_all(
        requests.reshape(shard_count, capacity), "user", split_axis=0, concat_axis=0, tiled=True
    )
    safe_rows = jnp.maximum(received.reshape(-1), 0)
    looked_up = item_table[safe_rows].reshape(shard_count, capacity, model_width)
    returned = lax.all_to_all(looked_up, "user", split_axis=0, concat_axis=0, tiled=True)
    embedded = returned.reshape(-1, model_width)[slot_index]
    projected = jnp.dot(
        embedded, w_qkvu.reshape(model_width, -1), preferred_element_type=jnp.float32
    )
    activated = jax.nn.silu(projected).astype(jnp.bfloat16)
    activated = activated.reshape(user_count, cand_count, heads_here, 4, head_size)
    queries = activated[:, :, :, 0]
    own_keys = activated[:, :, :, 1]
    own_values = activated[:, :, :, 2]
    gates = activated[:, :, :, 3]
    cached_keys = key_cache.reshape(user_count, prefix_most, heads_here, head_size)
    cached_values = value_cache.reshape(user_count, prefix_most, heads_here, head_size)
    raw = jnp.einsum("uchd,uphd->uhcp", queries, cached_keys, preferred_element_type=jnp.float32)
    denominator = (prefix_len + 1).astype(jnp.float32)
    in_prefix = jnp.arange(prefix_most, dtype=jnp.int32)[None, :] < prefix_len[:, None]
    weights = jnp.where(in_prefix[:, None, None, :], jax.nn.silu(raw * score_scale), 0.0)
    weights = (weights / denominator[:, None, None, None]).astype(jnp.bfloat16)
    attended = jnp.einsum(
        "uhcp,uphd->uchd", weights, cached_values, preferred_element_type=jnp.float32
    )
    own_dot = jnp.sum(queries.astype(jnp.float32) * own_keys.astype(jnp.float32), axis=-1)
    own_weight = jax.nn.silu(own_dot * score_scale) / denominator[:, None, None]
    attended = attended + own_weight[..., None] * own_values.astype(jnp.float32)
    mean_square = jnp.mean(attended * attended, axis=-1, keepdims=True)
    gated = (attended * lax.rsqrt(mean_square + 1e-06) * gates.astype(jnp.float32)).astype(
        jnp.bfloat16
    )
    partial_value = jnp.dot(
        gated.reshape(row_count, heads_here * head_size),
        w_out.reshape(heads_here * head_size, model_width),
        preferred_element_type=jnp.float32,
    )
    col_width = model_width // lax.axis_size("head")
    head_index = lax.axis_index("head")
    summed_cols = lax.psum_scatter(
        partial_value.astype(jnp.bfloat16), "head", scatter_dimension=1, tiled=True
    ).astype(jnp.float32)
    embed_cols = lax.dynamic_slice_in_dim(embedded, head_index * col_width, col_width, 1).astype(
        jnp.float32
    )
    square_part = jnp.sum(summed_cols * summed_cols, axis=1)
    inner_part = jnp.sum(summed_cols * embed_cols, axis=1)
    square_total, inner_total = lax.psum((square_part, inner_part), "head")
    scores_out = inner_total * model_width ** (-0.5) * lax.rsqrt(square_total / model_width + 1e-06)
    return scores_out.reshape(user_count, cand_count)


def solution(mesh):
    if fits_fused(mesh):
        return fused(mesh)
    in_specs = (
        P(("grp", "user"), None),
        P(("grp", "user")),
        P(("grp", "user"), None, "head"),
        P(("grp", "user"), None, "head"),
        P("user", None),
        P(None, "head", None, None),
        P("head", None, None),
    )
    out_specs = P(("grp", "user"), None)
    return jax.shard_map(body, mesh=mesh, in_specs=in_specs, out_specs=out_specs, check_vma=False)
```

```python
import functools

import jax
import jax.numpy as jnp
from jax import lax
from jax.experimental import pallas as pl
from jax.experimental.pallas import tpu as pltpu
from jax.sharding import PartitionSpec as P

MESH = pl.DeviceIdType.MESH
PIECES = 2
STRIP = 128


def silu(v):
    return v * (0.5 * jnp.tanh(0.5 * v) + 0.5)


def kernel(
    chips, prefix_ref, ids_ref, key_hbm, value_hbm, table_hbm, w_hbm, wout_hbm, out_ref,
    tab, ids_peer, ids_wide, picked, one_hot, emb, emb_peer, w_raw, w_wide, w, keys, values, wout, acc, gated,
    gated_peer, halves, local_sem, z_send, z_recv, ids_sem, exch_send, exch_recv, wout_sem, tail_sem,
):
    grp, user, head = lax.axis_index("grp"), lax.axis_index("user"), lax.axis_index("head")
    z, core = user // 2, user % 2
    sibling = user + 1 - 2 * core
    quarter = 2 * grp + head
    shards, rows, width = tab.shape
    cand = ids_ref.shape[1]
    half = cand // 2
    piece = rows // PIECES
    heads, head_size = wout_hbm.shape[0], wout_hbm.shape[1]
    here = heads * head_size
    prefix_most = keys.shape[0]
    model = w.shape[0]
    x_peer = (grp, user, 1 - head)
    y_peer = (1 - grp, user, head)
    corner = (1 - grp, user, 1 - head)

    own = pltpu.make_async_copy(
        table_hbm.at[:, pl.ds(pl.multiple_of(quarter * width, width), width)],
        tab.at[user], local_sem.at[0],
    )
    loads = [
        pltpu.make_async_copy(wout_hbm, wout.at[head], local_sem.at[1]),
        pltpu.make_async_copy(w_hbm, w_raw, local_sem.at[2]),
        pltpu.make_async_copy(key_hbm.at[0], keys, local_sem.at[3]),
        pltpu.make_async_copy(value_hbm.at[0], values, local_sem.at[4]),
    ]
    own.start()
    for load in loads:
        load.start()

    barrier = pltpu.get_barrier_semaphore()

    def greet(device):
        pl.semaphore_signal(barrier, inc=1, device_id=device, device_id_type=MESH)

    for device in ((grp, sibling, head), x_peer, y_peer, corner):
        greet(device)

    @pl.when(z > 0)
    def _():
        greet((grp, user - 2, head))

    @pl.when(z < chips - 1)
    def _():
        greet((grp, user + 2, head))

    pl.semaphore_wait(barrier, 4 + jnp.minimum(z, 1) + jnp.minimum(chips - 1 - z, 1))

    def remote(src, dst, send, recv, device):
        return pltpu.make_async_remote_copy(
            src_ref=src, dst_ref=dst, send_sem=send, recv_sem=recv, device_id=device,
            device_id_type=MESH,
        )

    def block(chip, parity, part):
        return tab.at[2 * chip + parity, pl.ds(part * piece, piece)]

    def along(chip, part, step):
        place = block(chip, core, part)
        return remote(
            place, place, z_send.at[0 if step > 0 else 1, chip, part], z_recv.at[0, chip, part],
            (grp, user + 2 * step, head),
        )

    def across(chip, part, parity):
        place = block(chip, parity, part)
        return remote(
            place, place, z_send.at[2, chip, part], z_recv.at[1, chip, part],
            (grp, sibling, head),
        )

    def when(condition, action):
        pl.when(condition)(action)

    ids_copy = remote(ids_ref, ids_peer, ids_sem.at[0], ids_sem.at[1], y_peer)
    ids_copy.start()
    own.wait()
    for part in range(PIECES):
        when(z < chips - 1, lambda: along(z, part, 1).start())
        when(z > 0, lambda: along(z, part, -1).start())
        across(z, part, core).start()
    loads[0].wait()
    wout_copies = []
    depth = head_size * heads // 2

    def wout_part(group, part):
        return wout.at[group, pl.ds(pl.multiple_of(part * (heads // 2), heads // 2), heads // 2)]

    to_peer = remote(wout_part(head, core), wout_part(head, core), wout_sem.at[0], wout_sem.at[1], x_peer)
    to_peer.start()
    ids_copy.wait()

    lane = lax.broadcasted_iota(jnp.int32, (cand, 128), 1)
    down = lax.broadcasted_iota(jnp.int32, (cand, cand), 0)
    diagonal = down == lax.broadcasted_iota(jnp.int32, (cand, cand), 1)
    place_row = None
    for which, source in enumerate((ids_ref, ids_peer)):
        ids = source[...]
        chip_of = sum((ids >= k * 2 * rows).astype(jnp.int32) for k in range(1, chips))
        key_row = (
            jnp.abs(chip_of - z) * cand + lax.broadcasted_iota(jnp.int32, (1, cand), 1)
        ).astype(jnp.float32)
        key_column = jnp.sum(jnp.where(diagonal, key_row, 0.0), axis=1, keepdims=True)
        place = jnp.sum(
            jnp.where(key_column < key_row, 1.0, 0.0), axis=0, keepdims=True
        ).astype(jnp.int32)
        ordered = jnp.sum(
            jnp.where(place == down, ids.astype(jnp.float32), 0.0), axis=1, keepdims=True
        ).astype(jnp.int32)
        ids_wide[which] = jnp.broadcast_to(ordered, (cand, 128))
        if which == 0:
            place_row = place
    picked[...] = jnp.zeros_like(picked)

    def mark(chip, low):
        def step(i, carry):
            wide = ids_wide[i // 2, low:] - (2 * chip + i % 2) * rows
            for j in range(rows // 128):
                one_hot[i, low:, j * 128 : (j + 1) * 128] = jnp.where(
                    wide == lane[low:] + j * 128, 1.0, 0.0
                ).astype(jnp.bfloat16)
            return carry

        lax.fori_loop(0, 4, step, 0)

    def pick(chip, low):
        def step(i, carry):
            picked[i // 2, low:] += jnp.dot(
                one_hot[i, low:], tab[2 * chip + i % 2], preferred_element_type=jnp.float32
            )
            return carry

        lax.fori_loop(0, 4, step, 0)

    def wait_sibling(chip):
        for part in range(PIECES):
            across(chip, part, 1 - core).wait_recv()

    def take(chip):
        mark(chip, 0)
        wait_sibling(chip)
        pick(chip, 0)

    def take_valid(chip):
        pl.when(jnp.logical_and(chip >= 0, chip < chips))(lambda: take(chip))

    slots = heads * 4
    strips = model // STRIP

    def spread(i, carry):
        start = pl.multiple_of(i * STRIP * slots, STRIP * slots)
        w_wide[...] = w_raw[pl.ds(start, STRIP * slots)].astype(jnp.float32)
        for j in range(slots):
            w[pl.ds(pl.multiple_of(i * STRIP, STRIP), STRIP), j * head_size : (j + 1) * head_size] = (
                w_wide[pl.ds(j, STRIP, stride=slots)].astype(jnp.bfloat16)
            )
        return carry

    def weight(which, h):
        return w[
            pl.ds(pl.multiple_of(which * width, width), width),
            pl.ds(pl.multiple_of(h * 4 * head_size, 4 * head_size), 4 * head_size),
        ]

    def embedded(which, start, count):
        return emb[which, pl.ds(pl.multiple_of(start, count), count)]

    def project(which, start, count, h):
        return jnp.dot(
            embedded(which, start, count), weight(which, h), preferred_element_type=jnp.float32
        )

    def swaps(r):
        span = pl.ds(r * half, half)
        mine, other = emb.at[quarter, span], emb_peer.at[span]
        return [
            remote(mine, mine, exch_send.at[r, 0], exch_recv.at[r, quarter], x_peer),
            remote(other, mine, exch_send.at[r, 1], exch_recv.at[r, quarter], y_peer),
            remote(other, mine, exch_send.at[r, 2], exch_recv.at[r, quarter], corner),
        ]

    def hand_out(r):
        emb_peer[r * half : (r + 1) * half] = picked[1, r * half : (r + 1) * half].astype(jnp.bfloat16)
        emb[quarter, r * half : (r + 1) * half] = picked[0, r * half : (r + 1) * half].astype(
            jnp.bfloat16
        )
        for copy in swaps(r):
            copy.start()

        def first(h, carry):
            acc[r, h] = project(quarter, r * half, half, h)
            return carry

        lax.fori_loop(0, heads, first, 0)

    at_end = jnp.logical_or(z == 0, z == chips - 1)
    inside = jnp.logical_and(z > 0, z < chips - 1)
    near = 1 - 2 * jnp.minimum(z, 1)
    take(z)
    loads[1].wait()
    lax.fori_loop(0, 3 * strips // 8, spread, 0)
    for distance in range(1, chips):
        for part in range(PIECES):

            @pl.when(z - distance >= 0)
            def _():
                along(z - distance, part, 1).wait_recv()
                when(z < chips - 1, lambda: along(z - distance, part, 1).start())
                across(z - distance, part, core).start()

            @pl.when(z + distance < chips)
            def _():
                along(z + distance, part, -1).wait_recv()
                when(z > 0, lambda: along(z + distance, part, -1).start())
                across(z + distance, part, core).start()

            if part == 0:
                if distance == 1:
                    lax.fori_loop(3 * strips // 8, 5 * strips // 8, spread, 0)
                else:
                    take_valid(z - near * (distance - 1))
                if distance == chips - 2:
                    lax.fori_loop(6 * strips // 8, strips, spread, 0)
                    when(inside, lambda: hand_out(0))
            elif part == PIECES - 1:
                if distance < chips - 1:
                    take_valid(z + near * distance)
                if distance == 1:
                    lax.fori_loop(5 * strips // 8, 6 * strips // 8, spread, 0)
                if distance == chips - 2:

                    @pl.when(at_end)
                    def _():
                        hand_out(0)
                        mark(z + near * (chips - 1), half)

    @pl.when(at_end)
    def _():
        wait_sibling(z + near * (chips - 1))
        pick(z + near * (chips - 1), half)

    hand_out(1)
    to_peer.wait()
    forward = remote(
        wout_part(1 - head, core), wout_part(1 - head, core), wout_sem.at[2], wout_sem.at[3],
        (grp, sibling, head),
    )
    forward.start()
    for load in loads[2:]:
        load.wait()

    others = (2 * grp + 1 - head, 2 * (1 - grp) + head, 2 * (1 - grp) + 1 - head)

    def arrived(r):
        for which in others:
            place = emb.at[which, pl.ds(r * half, half)]
            remote(place, place, exch_send.at[r, 0], exch_recv.at[r, which], x_peer).wait_recv()

    length = prefix_ref[0]
    inverse = 1.0 / (length + 1).astype(jnp.float32)
    in_prefix = lax.broadcasted_iota(jnp.int32, (1, prefix_most), 1) < length
    factor = jnp.where(in_prefix, inverse, 0.0)
    scale = head_size ** (-0.5)

    def attend(r, offset, count):
        here_rows = pl.ds(pl.multiple_of(offset, count), count)

        def step(h, carry):
            projected = acc[r, h, here_rows]
            for which in others:
                projected += project(which, r * half + offset, count, h)
            activated = silu(projected).astype(jnp.bfloat16)
            query, own_key, own_value, gate = (
                activated[:, j * head_size : (j + 1) * head_size] for j in range(4)
            )
            columns = pl.ds(pl.multiple_of(h * head_size, head_size), head_size)
            raw = lax.dot_general(
                query, keys[:, columns], (((1,), (1,)), ((), ())),
                preferred_element_type=jnp.float32,
            )
            weights = (silu(raw * scale) * factor).astype(jnp.bfloat16)
            attended = jnp.dot(weights, values[:, columns], preferred_element_type=jnp.float32)
            own_dot = jnp.sum(
                query.astype(jnp.float32) * own_key.astype(jnp.float32), axis=1, keepdims=True
            )
            attended += silu(own_dot * scale) * inverse * own_value.astype(jnp.float32)
            mean_square = jnp.mean(attended * attended, axis=1, keepdims=True)
            gated[r, here_rows, columns] = (
                attended * lax.rsqrt(mean_square + 1e-06) * gate.astype(jnp.float32)
            ).astype(jnp.bfloat16)
            return carry

        lax.fori_loop(0, heads, step, 0)

    eighth = half // 2

    def hand_over(r):
        place = gated.at[r, pl.ds(pl.multiple_of((1 - head) * eighth, eighth), eighth)]
        return remote(place, gated_peer.at[r], tail_sem.at[r], tail_sem.at[2 + r], x_peer)

    def product(rows_here, group):
        return (
            jnp.dot(
                rows_here, wout[group].reshape(here, model), preferred_element_type=jnp.float32
            )
            .astype(jnp.bfloat16)
            .astype(jnp.float32)
        )

    def finish(r):
        offset = pl.multiple_of(head * eighth, eighth)
        summed = product(gated[r, pl.ds(offset, eighth)], head)
        hand_over(r).wait()
        summed += product(gated_peer[r], 1 - head)
        square = jnp.sum(summed * summed, axis=1, keepdims=True)
        inner = sum(
            jnp.sum(
                summed[:, i * width : (i + 1) * width]
                * embedded(i, r * half + offset, eighth).astype(jnp.float32),
                axis=1, keepdims=True,
            )
            for i in range(model // width)
        )
        score = inner * model ** (-0.5) * lax.rsqrt(square / model + 1e-06)
        slot = down[:eighth] + (r * half + offset)
        return jnp.sum(jnp.where(place_row == slot, score, 0.0), axis=0, keepdims=True)

    arrived(0)
    attend(0, 0, half)
    arrived(1)
    hand_over(0).start()
    attend(1, (1 - head) * eighth, eighth)
    hand_over(1).start()
    attend(1, head * eighth, eighth)
    forward.wait()
    early = finish(0)
    halves[head] = early + finish(1)
    last = remote(halves.at[head], halves.at[head], tail_sem.at[4], tail_sem.at[5], x_peer)
    last.start()
    for part in range(PIECES):
        for chip in range(chips):

            @pl.when(z < chips - 1)
            def _():
                when(chip <= z, lambda: along(chip, part, 1).wait_send())

            @pl.when(z > 0)
            def _():
                when(chip >= z, lambda: along(chip, part, -1).wait_send())

            across(chip, part, core).wait_send()
    for r in range(2):
        for copy in swaps(r):
            copy.wait_send()
    last.wait()
    out_ref[...] = halves[0] + halves[1]


def fused_body(mesh, cand_ids, prefix_len, key_cache, value_cache, item_table, w_qkvu, w_out):
    cand = cand_ids.shape[1]
    rows, model = item_table.shape
    heads, head_size = w_qkvu.shape[1], w_qkvu.shape[3]
    prefix_most, here = key_cache.shape[1:]
    shards = mesh.shape["user"]
    chips = shards // 2
    width = model // 4
    half = cand // 2
    hbm = pl.BlockSpec(memory_space=pl.ANY)
    bf16, f32 = jnp.bfloat16, jnp.float32
    return pl.pallas_call(
        functools.partial(kernel, chips),
        out_shape=jax.ShapeDtypeStruct((1, cand), f32),
        in_specs=[
            pl.BlockSpec(memory_space=pltpu.SMEM), pl.BlockSpec(memory_space=pltpu.VMEM),
            hbm, hbm, hbm, hbm, hbm,
        ],
        out_specs=pl.BlockSpec(memory_space=pltpu.VMEM),
        scratch_shapes=[
            pltpu.VMEM((shards, rows, width), bf16),
            pltpu.VMEM((1, cand), jnp.int32),
            pltpu.VMEM((2, cand, 128), jnp.int32),
            pltpu.VMEM((2, cand, width), f32),
            pltpu.VMEM((4, cand, rows), bf16),
            pltpu.VMEM((4, cand, width), bf16),
            pltpu.VMEM((cand, width), bf16),
            pltpu.VMEM((model * heads * 4, head_size), bf16),
            pltpu.VMEM((STRIP * heads * 4, head_size), f32),
            pltpu.VMEM((model, heads * 4 * head_size), bf16),
            pltpu.VMEM((prefix_most, here), bf16),
            pltpu.VMEM((prefix_most, here), bf16),
            pltpu.VMEM((2, heads, head_size, model), bf16),
            pltpu.VMEM((2, heads, half, 4 * head_size), f32),
            pltpu.VMEM((2, half, here), bf16),
            pltpu.VMEM((2, half // 2, here), bf16),
            pltpu.VMEM((2, 1, cand), f32),
            pltpu.SemaphoreType.DMA((5,)),
            pltpu.SemaphoreType.DMA((3, chips, PIECES)),
            pltpu.SemaphoreType.DMA((2, chips, PIECES)),
            pltpu.SemaphoreType.DMA((2,)),
            pltpu.SemaphoreType.DMA((2, 3)),
            pltpu.SemaphoreType.DMA((2, 4)),
            pltpu.SemaphoreType.DMA((4,)),
            pltpu.SemaphoreType.DMA((6,)),
        ],
        compiler_params=pltpu.CompilerParams(
            collective_id=0, has_side_effects=True, vmem_limit_bytes=60 * 1024 * 1024
        ),
    )(
        prefix_len, cand_ids, key_cache, value_cache, item_table,
        w_qkvu.reshape(model * heads * 4, head_size), w_out,
    )


def fits_fused(mesh):
    shape = mesh.shape
    return shape["grp"] == 2 and shape["head"] == 2 and shape["user"] == 8


def fused(mesh):
    in_specs = (
        P(("grp", "user"), None),
        P(("grp", "user")),
        P(("grp", "user"), None, "head"),
        P(("grp", "user"), None, "head"),
        P("user", None),
        P(None, "head", None, None),
        P("head", None, None),
    )
    return jax.shard_map(
        functools.partial(fused_body, mesh), mesh=mesh, in_specs=in_specs,
        out_specs=P(("grp", "user"), None), check_vma=False,
    )


def body(cand_ids, prefix_len, key_cache, value_cache, item_table, w_qkvu, w_out):
    user_count, cand_count = cand_ids.shape
    model_width = item_table.shape[1]
    heads_here = w_qkvu.shape[1]
    head_size = w_qkvu.shape[3]
    prefix_most = key_cache.shape[1]
    score_scale = head_size ** (-0.5)
    shard_count = lax.axis_size("user")
    rows_shard = item_table.shape[0]
    item_ids = cand_ids.reshape(-1)
    row_count = item_ids.shape[0]
    capacity = 2 * row_count // shard_count
    shard_of = item_ids // rows_shard
    local_row = item_ids - shard_of * rows_shard
    one_hot = (shard_of[:, None] == jnp.arange(shard_count, dtype=jnp.int32)[None, :]).astype(
        jnp.int32
    )
    position = jnp.sum((jnp.cumsum(one_hot, axis=0) - 1) * one_hot, axis=1)
    slot_index = shard_of * capacity + position
    requests = jnp.full((shard_count * capacity,), -1, jnp.int32).at[slot_index].set(local_row)
    received = lax.all_to_all(
        requests.reshape(shard_count, capacity), "user", split_axis=0, concat_axis=0, tiled=True
    )
    safe_rows = jnp.maximum(received.reshape(-1), 0)
    looked_up = item_table[safe_rows].reshape(shard_count, capacity, model_width)
    returned = lax.all_to_all(looked_up, "user", split_axis=0, concat_axis=0, tiled=True)
    embedded = returned.reshape(-1, model_width)[slot_index]
    projected = jnp.dot(
        embedded, w_qkvu.reshape(model_width, -1), preferred_element_type=jnp.float32
    )
    activated = jax.nn.silu(projected).astype(jnp.bfloat16)
    activated = activated.reshape(user_count, cand_count, heads_here, 4, head_size)
    queries = activated[:, :, :, 0]
    own_keys = activated[:, :, :, 1]
    own_values = activated[:, :, :, 2]
    gates = activated[:, :, :, 3]
    cached_keys = key_cache.reshape(user_count, prefix_most, heads_here, head_size)
    cached_values = value_cache.reshape(user_count, prefix_most, heads_here, head_size)
    raw = jnp.einsum("uchd,uphd->uhcp", queries, cached_keys, preferred_element_type=jnp.float32)
    denominator = (prefix_len + 1).astype(jnp.float32)
    in_prefix = jnp.arange(prefix_most, dtype=jnp.int32)[None, :] < prefix_len[:, None]
    weights = jnp.where(in_prefix[:, None, None, :], jax.nn.silu(raw * score_scale), 0.0)
    weights = (weights / denominator[:, None, None, None]).astype(jnp.bfloat16)
    attended = jnp.einsum(
        "uhcp,uphd->uchd", weights, cached_values, preferred_element_type=jnp.float32
    )
    own_dot = jnp.sum(queries.astype(jnp.float32) * own_keys.astype(jnp.float32), axis=-1)
    own_weight = jax.nn.silu(own_dot * score_scale) / denominator[:, None, None]
    attended = attended + own_weight[..., None] * own_values.astype(jnp.float32)
    mean_square = jnp.mean(attended * attended, axis=-1, keepdims=True)
    gated = (attended * lax.rsqrt(mean_square + 1e-06) * gates.astype(jnp.float32)).astype(
        jnp.bfloat16
    )
    partial_value = jnp.dot(
        gated.reshape(row_count, heads_here * head_size),
        w_out.reshape(heads_here * head_size, model_width),
        preferred_element_type=jnp.float32,
    )
    col_width = model_width // lax.axis_size("head")
    head_index = lax.axis_index("head")
    summed_cols = lax.psum_scatter(
        partial_value.astype(jnp.bfloat16), "head", scatter_dimension=1, tiled=True
    ).astype(jnp.float32)
    embed_cols = lax.dynamic_slice_in_dim(embedded, head_index * col_width, col_width, 1).astype(
        jnp.float32
    )
    square_part = jnp.sum(summed_cols * summed_cols, axis=1)
    inner_part = jnp.sum(summed_cols * embed_cols, axis=1)
    square_total, inner_total = lax.psum((square_part, inner_part), "head")
    scores_out = inner_total * model_width ** (-0.5) * lax.rsqrt(square_total / model_width + 1e-06)
    return scores_out.reshape(user_count, cand_count)


def solution(mesh):
    if fits_fused(mesh):
        return fused(mesh)
    in_specs = (
        P(("grp", "user"), None),
        P(("grp", "user")),
        P(("grp", "user"), None, "head"),
        P(("grp", "user"), None, "head"),
        P("user", None),
        P(None, "head", None, None),
        P("head", None, None),
    )
    out_specs = P(("grp", "user"), None)
    return jax.shard_map(body, mesh=mesh, in_specs=in_specs, out_specs=out_specs, check_vma=False)
```

```python
import functools

import jax
import jax.numpy as jnp
from jax import lax
from jax.experimental import pallas as pl
from jax.experimental.pallas import tpu as pltpu
from jax.sharding import PartitionSpec as P

MESH = pl.DeviceIdType.MESH
PIECES = 4
STRIP = 128


def silu(v):
    return v * (0.5 * jnp.tanh(0.5 * v) + 0.5)


def kernel(
    chips, prefix_ref, ids_ref, key_hbm, value_hbm, table_hbm, w_hbm, wout_hbm, out_ref,
    tab, ids_peer, ids_wide, picked, one_hot, emb, emb_peer, w_raw, w_wide, w, keys, values, wout, acc, gated,
    gated_peer, halves, local_sem, z_send, z_recv, ids_sem, exch_send, exch_recv, wout_sem, tail_sem,
):
    grp, user, head = lax.axis_index("grp"), lax.axis_index("user"), lax.axis_index("head")
    z, core = user // 2, user % 2
    sibling = user + 1 - 2 * core
    quarter = 2 * grp + head
    shards, rows, width = tab.shape
    cand = ids_ref.shape[1]
    half = cand // 2
    piece = rows // PIECES
    heads, head_size = wout_hbm.shape[0], wout_hbm.shape[1]
    here = heads * head_size
    prefix_most = keys.shape[0]
    model = w.shape[0]
    x_peer = (grp, user, 1 - head)
    y_peer = (1 - grp, user, head)
    corner = (1 - grp, user, 1 - head)

    own = pltpu.make_async_copy(
        table_hbm.at[:, pl.ds(pl.multiple_of(quarter * width, width), width)],
        tab.at[user], local_sem.at[0],
    )
    loads = [
        pltpu.make_async_copy(wout_hbm, wout.at[head], local_sem.at[1]),
        pltpu.make_async_copy(w_hbm, w_raw, local_sem.at[2]),
        pltpu.make_async_copy(key_hbm.at[0], keys, local_sem.at[3]),
        pltpu.make_async_copy(value_hbm.at[0], values, local_sem.at[4]),
    ]
    own.start()
    for load in loads:
        load.start()

    barrier = pltpu.get_barrier_semaphore()

    def greet(device):
        pl.semaphore_signal(barrier, inc=1, device_id=device, device_id_type=MESH)

    for device in ((grp, sibling, head), x_peer, y_peer, corner):
        greet(device)

    @pl.when(z > 0)
    def _():
        greet((grp, user - 2, head))

    @pl.when(z < chips - 1)
    def _():
        greet((grp, user + 2, head))

    pl.semaphore_wait(barrier, 4 + jnp.minimum(z, 1) + jnp.minimum(chips - 1 - z, 1))

    def remote(src, dst, send, recv, device):
        return pltpu.make_async_remote_copy(
            src_ref=src, dst_ref=dst, send_sem=send, recv_sem=recv, device_id=device,
            device_id_type=MESH,
        )

    def block(chip, parity, part):
        return tab.at[2 * chip + parity, pl.ds(part * piece, piece)]

    def along(chip, part, step):
        place = block(chip, core, part)
        return remote(
            place, place, z_send.at[0 if step > 0 else 1, chip, part], z_recv.at[0, chip, part],
            (grp, user + 2 * step, head),
        )

    def across(chip, part, parity):
        place = block(chip, parity, part)
        return remote(
            place, place, z_send.at[2, chip, part], z_recv.at[1, chip, part],
            (grp, sibling, head),
        )

    def when(condition, action):
        pl.when(condition)(action)

    ids_copy = remote(ids_ref, ids_peer, ids_sem.at[0], ids_sem.at[1], y_peer)
    ids_copy.start()
    own.wait()
    for part in range(PIECES):
        when(z < chips - 1, lambda: along(z, part, 1).start())
        when(z > 0, lambda: along(z, part, -1).start())
        across(z, part, core).start()
    loads[0].wait()
    wout_copies = []
    depth = head_size * heads // 2

    def wout_part(group, part):
        return wout.at[group, pl.ds(pl.multiple_of(part * (heads // 2), heads // 2), heads // 2)]

    to_peer = remote(wout_part(head, core), wout_part(head, core), wout_sem.at[0], wout_sem.at[1], x_peer)
    to_peer.start()
    ids_copy.wait()

    lane = lax.broadcasted_iota(jnp.int32, (cand, 128), 1)
    down = lax.broadcasted_iota(jnp.int32, (cand, cand), 0)
    diagonal = down == lax.broadcasted_iota(jnp.int32, (cand, cand), 1)
    place_row = None
    for which, source in enumerate((ids_ref, ids_peer)):
        ids = source[...]
        chip_of = sum((ids >= k * 2 * rows).astype(jnp.int32) for k in range(1, chips))
        key_row = (
            jnp.abs(chip_of - z) * cand + lax.broadcasted_iota(jnp.int32, (1, cand), 1)
        ).astype(jnp.float32)
        key_column = jnp.sum(jnp.where(diagonal, key_row, 0.0), axis=1, keepdims=True)
        place = jnp.sum(
            jnp.where(key_column < key_row, 1.0, 0.0), axis=0, keepdims=True
        ).astype(jnp.int32)
        ordered = jnp.sum(
            jnp.where(place == down, ids.astype(jnp.float32), 0.0), axis=1, keepdims=True
        ).astype(jnp.int32)
        ids_wide[which] = jnp.broadcast_to(ordered, (cand, 128))
        if which == 0:
            place_row = place
    picked[...] = jnp.zeros_like(picked)

    def mark(chip, low):
        def step(i, carry):
            wide = ids_wide[i // 2, low:] - (2 * chip + i % 2) * rows
            for j in range(rows // 128):
                one_hot[i, low:, j * 128 : (j + 1) * 128] = jnp.where(
                    wide == lane[low:] + j * 128, 1.0, 0.0
                ).astype(jnp.bfloat16)
            return carry

        lax.fori_loop(0, 4, step, 0)

    def pick(chip, low):
        def step(i, carry):
            picked[i // 2, low:] += jnp.dot(
                one_hot[i, low:], tab[2 * chip + i % 2], preferred_element_type=jnp.float32
            )
            return carry

        lax.fori_loop(0, 4, step, 0)

    def wait_sibling(chip):
        for part in range(PIECES):
            across(chip, part, 1 - core).wait_recv()

    def take(chip):
        mark(chip, 0)
        wait_sibling(chip)
        pick(chip, 0)

    def take_valid(chip):
        pl.when(jnp.logical_and(chip >= 0, chip < chips))(lambda: take(chip))

    slots = heads * 4
    strips = model // STRIP

    def spread(i, carry):
        start = pl.multiple_of(i * STRIP * slots, STRIP * slots)
        w_wide[...] = w_raw[pl.ds(start, STRIP * slots)].astype(jnp.float32)
        for j in range(slots):
            w[pl.ds(pl.multiple_of(i * STRIP, STRIP), STRIP), j * head_size : (j + 1) * head_size] = (
                w_wide[pl.ds(j, STRIP, stride=slots)].astype(jnp.bfloat16)
            )
        return carry

    def weight(which, h):
        return w[
            pl.ds(pl.multiple_of(which * width, width), width),
            pl.ds(pl.multiple_of(h * 4 * head_size, 4 * head_size), 4 * head_size),
        ]

    def embedded(which, start, count):
        return emb[which, pl.ds(pl.multiple_of(start, count), count)]

    def project(which, start, count, h):
        return jnp.dot(
            embedded(which, start, count), weight(which, h), preferred_element_type=jnp.float32
        )

    def swaps(r):
        span = pl.ds(r * half, half)
        mine, other = emb.at[quarter, span], emb_peer.at[span]
        return [
            remote(mine, mine, exch_send.at[r, 0], exch_recv.at[r, quarter], x_peer),
            remote(other, mine, exch_send.at[r, 1], exch_recv.at[r, quarter], y_peer),
            remote(other, mine, exch_send.at[r, 2], exch_recv.at[r, quarter], corner),
        ]

    def hand_out(r):
        emb_peer[r * half : (r + 1) * half] = picked[1, r * half : (r + 1) * half].astype(jnp.bfloat16)
        emb[quarter, r * half : (r + 1) * half] = picked[0, r * half : (r + 1) * half].astype(
            jnp.bfloat16
        )
        for copy in swaps(r):
            copy.start()

        def first(h, carry):
            acc[r, h] = project(quarter, r * half, half, h)
            return carry

        lax.fori_loop(0, heads, first, 0)

    at_end = jnp.logical_or(z == 0, z == chips - 1)
    inside = jnp.logical_and(z > 0, z < chips - 1)
    near = 1 - 2 * jnp.minimum(z, 1)
    take(z)
    loads[1].wait()
    lax.fori_loop(0, 3 * strips // 8, spread, 0)
    for distance in range(1, chips):
        for part in range(PIECES):

            @pl.when(z - distance >= 0)
            def _():
                along(z - distance, part, 1).wait_recv()
                when(z < chips - 1, lambda: along(z - distance, part, 1).start())
                across(z - distance, part, core).start()

            @pl.when(z + distance < chips)
            def _():
                along(z + distance, part, -1).wait_recv()
                when(z > 0, lambda: along(z + distance, part, -1).start())
                across(z + distance, part, core).start()

            if part == 0:
                if distance == 1:
                    lax.fori_loop(3 * strips // 8, 5 * strips // 8, spread, 0)
                else:
                    take_valid(z - near * (distance - 1))
                if distance == chips - 2:
                    lax.fori_loop(6 * strips // 8, strips, spread, 0)
                    when(inside, lambda: hand_out(0))
            elif part == PIECES - 1:
                if distance < chips - 1:
                    take_valid(z + near * distance)
                if distance == 1:
                    lax.fori_loop(5 * strips // 8, 6 * strips // 8, spread, 0)
                if distance == chips - 2:

                    @pl.when(at_end)
                    def _():
                        hand_out(0)
                        mark(z + near * (chips - 1), half)

    @pl.when(at_end)
    def _():
        wait_sibling(z + near * (chips - 1))
        pick(z + near * (chips - 1), half)

    hand_out(1)
    to_peer.wait()
    forward = remote(
        wout_part(1 - head, core), wout_part(1 - head, core), wout_sem.at[2], wout_sem.at[3],
        (grp, sibling, head),
    )
    forward.start()
    for load in loads[2:]:
        load.wait()

    others = (2 * grp + 1 - head, 2 * (1 - grp) + head, 2 * (1 - grp) + 1 - head)

    def arrived(r):
        for which in others:
            place = emb.at[which, pl.ds(r * half, half)]
            remote(place, place, exch_send.at[r, 0], exch_recv.at[r, which], x_peer).wait_recv()

    length = prefix_ref[0]
    inverse = 1.0 / (length + 1).astype(jnp.float32)
    in_prefix = lax.broadcasted_iota(jnp.int32, (1, prefix_most), 1) < length
    factor = jnp.where(in_prefix, inverse, 0.0)
    scale = head_size ** (-0.5)

    def attend(r, offset, count):
        here_rows = pl.ds(pl.multiple_of(offset, count), count)

        def step(h, carry):
            projected = acc[r, h, here_rows]
            for which in others:
                projected += project(which, r * half + offset, count, h)
            activated = silu(projected).astype(jnp.bfloat16)
            query, own_key, own_value, gate = (
                activated[:, j * head_size : (j + 1) * head_size] for j in range(4)
            )
            columns = pl.ds(pl.multiple_of(h * head_size, head_size), head_size)
            raw = lax.dot_general(
                query, keys[:, columns], (((1,), (1,)), ((), ())),
                preferred_element_type=jnp.float32,
            )
            weights = (silu(raw * scale) * factor).astype(jnp.bfloat16)
            attended = jnp.dot(weights, values[:, columns], preferred_element_type=jnp.float32)
            own_dot = jnp.sum(
                query.astype(jnp.float32) * own_key.astype(jnp.float32), axis=1, keepdims=True
            )
            attended += silu(own_dot * scale) * inverse * own_value.astype(jnp.float32)
            mean_square = jnp.mean(attended * attended, axis=1, keepdims=True)
            gated[r, here_rows, columns] = (
                attended * lax.rsqrt(mean_square + 1e-06) * gate.astype(jnp.float32)
            ).astype(jnp.bfloat16)
            return carry

        lax.fori_loop(0, heads, step, 0)

    eighth = half // 2

    def hand_over(r):
        place = gated.at[r, pl.ds(pl.multiple_of((1 - head) * eighth, eighth), eighth)]
        return remote(place, gated_peer.at[r], tail_sem.at[r], tail_sem.at[2 + r], x_peer)

    def product(rows_here, group):
        return (
            jnp.dot(
                rows_here, wout[group].reshape(here, model), preferred_element_type=jnp.float32
            )
            .astype(jnp.bfloat16)
            .astype(jnp.float32)
        )

    def finish(r):
        offset = pl.multiple_of(head * eighth, eighth)
        summed = product(gated[r, pl.ds(offset, eighth)], head)
        hand_over(r).wait()
        summed += product(gated_peer[r], 1 - head)
        square = jnp.sum(summed * summed, axis=1, keepdims=True)
        inner = sum(
            jnp.sum(
                summed[:, i * width : (i + 1) * width]
                * embedded(i, r * half + offset, eighth).astype(jnp.float32),
                axis=1, keepdims=True,
            )
            for i in range(model // width)
        )
        score = inner * model ** (-0.5) * lax.rsqrt(square / model + 1e-06)
        slot = down[:eighth] + (r * half + offset)
        return jnp.sum(jnp.where(place_row == slot, score, 0.0), axis=0, keepdims=True)

    arrived(0)
    attend(0, 0, half)
    arrived(1)
    hand_over(0).start()
    attend(1, (1 - head) * eighth, eighth)
    hand_over(1).start()
    attend(1, head * eighth, eighth)
    forward.wait()
    early = finish(0)
    halves[head] = early + finish(1)
    last = remote(halves.at[head], halves.at[head], tail_sem.at[4], tail_sem.at[5], x_peer)
    last.start()
    for part in range(PIECES):
        for chip in range(chips):

            @pl.when(z < chips - 1)
            def _():
                when(chip <= z, lambda: along(chip, part, 1).wait_send())

            @pl.when(z > 0)
            def _():
                when(chip >= z, lambda: along(chip, part, -1).wait_send())

            across(chip, part, core).wait_send()
    for r in range(2):
        for copy in swaps(r):
            copy.wait_send()
    last.wait()
    out_ref[...] = halves[0] + halves[1]


def fused_body(mesh, cand_ids, prefix_len, key_cache, value_cache, item_table, w_qkvu, w_out):
    cand = cand_ids.shape[1]
    rows, model = item_table.shape
    heads, head_size = w_qkvu.shape[1], w_qkvu.shape[3]
    prefix_most, here = key_cache.shape[1:]
    shards = mesh.shape["user"]
    chips = shards // 2
    width = model // 4
    half = cand // 2
    hbm = pl.BlockSpec(memory_space=pl.ANY)
    bf16, f32 = jnp.bfloat16, jnp.float32
    return pl.pallas_call(
        functools.partial(kernel, chips),
        out_shape=jax.ShapeDtypeStruct((1, cand), f32),
        in_specs=[
            pl.BlockSpec(memory_space=pltpu.SMEM), pl.BlockSpec(memory_space=pltpu.VMEM),
            hbm, hbm, hbm, hbm, hbm,
        ],
        out_specs=pl.BlockSpec(memory_space=pltpu.VMEM),
        scratch_shapes=[
            pltpu.VMEM((shards, rows, width), bf16),
            pltpu.VMEM((1, cand), jnp.int32),
            pltpu.VMEM((2, cand, 128), jnp.int32),
            pltpu.VMEM((2, cand, width), f32),
            pltpu.VMEM((4, cand, rows), bf16),
            pltpu.VMEM((4, cand, width), bf16),
            pltpu.VMEM((cand, width), bf16),
            pltpu.VMEM((model * heads * 4, head_size), bf16),
            pltpu.VMEM((STRIP * heads * 4, head_size), f32),
            pltpu.VMEM((model, heads * 4 * head_size), bf16),
            pltpu.VMEM((prefix_most, here), bf16),
            pltpu.VMEM((prefix_most, here), bf16),
            pltpu.VMEM((2, heads, head_size, model), bf16),
            pltpu.VMEM((2, heads, half, 4 * head_size), f32),
            pltpu.VMEM((2, half, here), bf16),
            pltpu.VMEM((2, half // 2, here), bf16),
            pltpu.VMEM((2, 1, cand), f32),
            pltpu.SemaphoreType.DMA((5,)),
            pltpu.SemaphoreType.DMA((3, chips, PIECES)),
            pltpu.SemaphoreType.DMA((2, chips, PIECES)),
            pltpu.SemaphoreType.DMA((2,)),
            pltpu.SemaphoreType.DMA((2, 3)),
            pltpu.SemaphoreType.DMA((2, 4)),
            pltpu.SemaphoreType.DMA((4,)),
            pltpu.SemaphoreType.DMA((6,)),
        ],
        compiler_params=pltpu.CompilerParams(
            collective_id=0, has_side_effects=True, vmem_limit_bytes=60 * 1024 * 1024
        ),
    )(
        prefix_len, cand_ids, key_cache, value_cache, item_table,
        w_qkvu.reshape(model * heads * 4, head_size), w_out,
    )


def fits_fused(mesh):
    shape = mesh.shape
    return shape["grp"] == 2 and shape["head"] == 2 and shape["user"] == 8


def fused(mesh):
    in_specs = (
        P(("grp", "user"), None),
        P(("grp", "user")),
        P(("grp", "user"), None, "head"),
        P(("grp", "user"), None, "head"),
        P("user", None),
        P(None, "head", None, None),
        P("head", None, None),
    )
    return jax.shard_map(
        functools.partial(fused_body, mesh), mesh=mesh, in_specs=in_specs,
        out_specs=P(("grp", "user"), None), check_vma=False,
    )


def body(cand_ids, prefix_len, key_cache, value_cache, item_table, w_qkvu, w_out):
    user_count, cand_count = cand_ids.shape
    model_width = item_table.shape[1]
    heads_here = w_qkvu.shape[1]
    head_size = w_qkvu.shape[3]
    prefix_most = key_cache.shape[1]
    score_scale = head_size ** (-0.5)
    shard_count = lax.axis_size("user")
    rows_shard = item_table.shape[0]
    item_ids = cand_ids.reshape(-1)
    row_count = item_ids.shape[0]
    capacity = 2 * row_count // shard_count
    shard_of = item_ids // rows_shard
    local_row = item_ids - shard_of * rows_shard
    one_hot = (shard_of[:, None] == jnp.arange(shard_count, dtype=jnp.int32)[None, :]).astype(
        jnp.int32
    )
    position = jnp.sum((jnp.cumsum(one_hot, axis=0) - 1) * one_hot, axis=1)
    slot_index = shard_of * capacity + position
    requests = jnp.full((shard_count * capacity,), -1, jnp.int32).at[slot_index].set(local_row)
    received = lax.all_to_all(
        requests.reshape(shard_count, capacity), "user", split_axis=0, concat_axis=0, tiled=True
    )
    safe_rows = jnp.maximum(received.reshape(-1), 0)
    looked_up = item_table[safe_rows].reshape(shard_count, capacity, model_width)
    returned = lax.all_to_all(looked_up, "user", split_axis=0, concat_axis=0, tiled=True)
    embedded = returned.reshape(-1, model_width)[slot_index]
    projected = jnp.dot(
        embedded, w_qkvu.reshape(model_width, -1), preferred_element_type=jnp.float32
    )
    activated = jax.nn.silu(projected).astype(jnp.bfloat16)
    activated = activated.reshape(user_count, cand_count, heads_here, 4, head_size)
    queries = activated[:, :, :, 0]
    own_keys = activated[:, :, :, 1]
    own_values = activated[:, :, :, 2]
    gates = activated[:, :, :, 3]
    cached_keys = key_cache.reshape(user_count, prefix_most, heads_here, head_size)
    cached_values = value_cache.reshape(user_count, prefix_most, heads_here, head_size)
    raw = jnp.einsum("uchd,uphd->uhcp", queries, cached_keys, preferred_element_type=jnp.float32)
    denominator = (prefix_len + 1).astype(jnp.float32)
    in_prefix = jnp.arange(prefix_most, dtype=jnp.int32)[None, :] < prefix_len[:, None]
    weights = jnp.where(in_prefix[:, None, None, :], jax.nn.silu(raw * score_scale), 0.0)
    weights = (weights / denominator[:, None, None, None]).astype(jnp.bfloat16)
    attended = jnp.einsum(
        "uhcp,uphd->uchd", weights, cached_values, preferred_element_type=jnp.float32
    )
    own_dot = jnp.sum(queries.astype(jnp.float32) * own_keys.astype(jnp.float32), axis=-1)
    own_weight = jax.nn.silu(own_dot * score_scale) / denominator[:, None, None]
    attended = attended + own_weight[..., None] * own_values.astype(jnp.float32)
    mean_square = jnp.mean(attended * attended, axis=-1, keepdims=True)
    gated = (attended * lax.rsqrt(mean_square + 1e-06) * gates.astype(jnp.float32)).astype(
        jnp.bfloat16
    )
    partial_value = jnp.dot(
        gated.reshape(row_count, heads_here * head_size),
        w_out.reshape(heads_here * head_size, model_width),
        preferred_element_type=jnp.float32,
    )
    col_width = model_width // lax.axis_size("head")
    head_index = lax.axis_index("head")
    summed_cols = lax.psum_scatter(
        partial_value.astype(jnp.bfloat16), "head", scatter_dimension=1, tiled=True
    ).astype(jnp.float32)
    embed_cols = lax.dynamic_slice_in_dim(embedded, head_index * col_width, col_width, 1).astype(
        jnp.float32
    )
    square_part = jnp.sum(summed_cols * summed_cols, axis=1)
    inner_part = jnp.sum(summed_cols * embed_cols, axis=1)
    square_total, inner_total = lax.psum((square_part, inner_part), "head")
    scores_out = inner_total * model_width ** (-0.5) * lax.rsqrt(square_total / model_width + 1e-06)
    return scores_out.reshape(user_count, cand_count)


def solution(mesh):
    if fits_fused(mesh):
        return fused(mesh)
    in_specs = (
        P(("grp", "user"), None),
        P(("grp", "user")),
        P(("grp", "user"), None, "head"),
        P(("grp", "user"), None, "head"),
        P("user", None),
        P(None, "head", None, None),
        P("head", None, None),
    )
    out_specs = P(("grp", "user"), None)
    return jax.shard_map(body, mesh=mesh, in_specs=in_specs, out_specs=out_specs, check_vma=False)
```
